256 devices in a mesh: branch: 32 (over y, z), tensor: 8 (over x, core).
Axes of the slice: x: 4, y: 4, z: 8, core: 2. Of those that a mesh axis runs over, the one named last changes fastest.
Arguments:
- layer_input: bfloat16 [16384, 5120], P(('branch', 'tensor')), may hold values from -360 to 360
- norm_gain: float32 [5120], replicated, may hold values from 0.25 to 1.75
- projection_weight: bfloat16 [5120, 5120], P(None, 'tensor'), may hold values from -0.078125 to 0.078125
- output_weight: bfloat16 [3072, 5120], P('tensor'), may hold values from -3 to 3
- prompt_cache: bfloat16 [2048, 2048], P(None, 'tensor'), may hold values from -1800 to 1800
- subtree_cache: bfloat16 [2, 16384, 2048], P(None, 'branch', 'tensor'), may hold values from -6 to 6
- parents: int32 [2, 32], replicated, may hold values from 0 to 31
- leaf_scores: float32 [32], P('branch'), may hold values from 0.3 to 1
Outputs:
- attn_output: bfloat16 [16384, 5120], P(('branch', 'tensor'))
- subtree_min: float32 [2, 32], P(None, 'branch')
- subtree_product: float32 [2, 32], P(None, 'branch')
The draws below stay inside these ranges and needn't reach their ends.
Inputs may be any that keep to these rules, and one draw needn't show every extreme that they name: parents[0, j] is the parent in level one of node j of level two; parents[1, j] is the parent in level two of new node j. Node j of every level is held by branch index j.
All inputs are finite; a program needn't handle non-finite values.
Results may differ from the reference program's by a relative error of at most 0.015.
Values may be sent and summed in bfloat16 or wider, within the bound.
No kernel may reach another device: no remote copies, remote signals or barrier semaphores. Data moves between devices by JAX's collectives and lax.ppermute only.
A program may use at most 128 MiB of HBM per device.

```python
import math
import jax
import jax.numpy as jnp
import numpy as np
from jax import lax

MODEL_WIDTH = 5120
KEY_VALUE_HEADS = 8
QUERY_GROUP = 3
HEAD_SIZE = 128
SEGMENT_TOKENS = 512
PROMPT_TOKENS = 2048
HQ = 24
LEVEL_NODES = 32
TOKENS = 16384
N_TENSOR = 8


def draw_layer_input(key, part):
    starting_key, column_key, scale_key = jax.random.split(key, 3)
    columns = jnp.exp(jax.random.uniform(column_key, (1, MODEL_WIDTH), jnp.float32, 0.0, math.log(10.0)))
    base_value = jnp.clip(jax.random.normal(starting_key, (TOKENS, MODEL_WIDTH), jnp.float32), -4.0, 4.0)
    scales = jnp.exp(jax.random.uniform(scale_key, (TOKENS, 1), jnp.float32, math.log(0.5), math.log(2.0)))
    return (base_value * columns * scales).astype(jnp.bfloat16)


def draw_prompt_cache(key, part):
    starting_key = jax.random.fold_in(key, 0)
    base_value = jnp.clip(jax.random.normal(starting_key, (PROMPT_TOKENS, KEY_VALUE_HEADS, 2, HEAD_SIZE), jnp.float32), -4.0, 4.0)
    return base_value.reshape(PROMPT_TOKENS, KEY_VALUE_HEADS * 2 * HEAD_SIZE).astype(jnp.bfloat16)


def place_ends(array, stream_key, smallest, top_value):
    shape = array.shape
    index_at = [jax.random.randint(jax.random.fold_in(stream_key, axis), (), 0, shape[axis]) for axis in range(len(shape))]
    array = array.at[tuple(index_at)].set(smallest)
    longest = shape.index(max(shape))
    index_at[longest] = (index_at[longest] + 1) % shape[longest]
    return array.at[tuple(index_at)].set(top_value)


def levels(rng, extent, cuts, smallest, largest):
    level, own = 1.0, jax.random.fold_in(rng, 6)
    for axis_at, parts in cuts:
        steps = jnp.exp(jax.random.uniform(jax.random.fold_in(own, axis_at), (parts,), jnp.float32, smallest / len(cuts), largest / len(cuts)))
        level = level * jnp.repeat(steps, extent[axis_at] // parts).reshape([-1 if axis == axis_at else 1 for axis in range(len(extent))])
    return level


def cumulative_ranks(amount, slope):
    loads = [(1 << 20) // math.isqrt(rank ** slope) + 1 for rank in range(1, amount + 1)]
    spread = 1 + sum(loads) // (1 << 30)
    return np.cumsum(np.array([max(1, weight // spread) for weight in loads]))


def skewed_ids(key, extent, amount, skew):
    listing = cumulative_ranks(amount, skew)
    lot = jax.random.randint(jax.random.fold_in(key, 1), extent, 0, int(listing[amount - 1]))
    rank = jnp.searchsorted(jnp.asarray(listing, jnp.int32), lot, side="right")
    return jax.random.permutation(jax.random.fold_in(key, 2), amount)[rank].astype(jnp.int32)


def noise(key, dims, deviation, bound, cuts=(), held_as=jnp.bfloat16):
    entries = jax.random.normal(key, dims, jnp.float32) * deviation
    if len(cuts) > 0:
        entries = levels(key, dims, cuts, -0.22, 0.18) * entries
    return jnp.clip(entries, min=-bound, max=bound).astype(held_as)


def setup_inputs(seed: int = 0) -> dict:
    key_list = jax.random.split(jax.random.key(seed), 9)
    layer_input = draw_layer_input(jax.random.fold_in(key_list[8], 71), 0)
    norm_gain = jnp.clip(1.0 + 0.15 * jax.random.normal(key_list[1], (MODEL_WIDTH,), jnp.float32), 0.25, 1.75)
    projection_weight = noise(key_list[2], (MODEL_WIDTH, KEY_VALUE_HEADS * (QUERY_GROUP + 2) * HEAD_SIZE), MODEL_WIDTH ** -0.5, 0.078125, ((1, 8),))
    output_weight = noise(key_list[3], (HQ * HEAD_SIZE, MODEL_WIDTH), 0.5, 3.0, ((0, 8),))
    prompt_cache = draw_prompt_cache(jax.random.fold_in(key_list[8], 71), 0)
    subtree_cache = noise(key_list[5], (2, LEVEL_NODES * SEGMENT_TOKENS, KEY_VALUE_HEADS * 2 * HEAD_SIZE), 1.0, 6.0, ((1, 32), (2, 8)))
    parents = place_ends(skewed_ids(key_list[6], (2, LEVEL_NODES), LEVEL_NODES, 2), jax.random.fold_in(key_list[6], 3), 0, LEVEL_NODES - 1).astype(jnp.int32)
    leaf_scores = jnp.clip(0.3 + 0.7 * jax.random.uniform(key_list[7], (LEVEL_NODES,), jnp.float32) ** levels(key_list[7], (LEVEL_NODES,), ((0, 32),), -0.2, 0.2), 0.3, 1.0)
    return {"layer_input": layer_input, "norm_gain": norm_gain, "projection_weight": projection_weight, "output_weight": output_weight, "prompt_cache": prompt_cache, "subtree_cache": subtree_cache, "parents": parents, "leaf_scores": leaf_scores}


THETA = 1000000.0
EPSILON = 1e-06

def normalize(inputs, gain):
    wide = inputs.astype(jnp.float32)
    scale = lax.rsqrt(lax.optimization_barrier(jnp.mean(wide * wide, axis=-1, keepdims=True)) + EPSILON)
    return (wide * scale * gain.astype(jnp.float32)).astype(jnp.bfloat16)

def rotate(vectors, offset):
    half = vectors.shape[-1] // 2
    freq = THETA ** (-jnp.arange(half, dtype=jnp.float32) * 2.0 / vectors.shape[-1])
    places = (offset + jnp.arange(vectors.shape[0])).astype(jnp.float32)
    angle = places[:, None] * freq[None, :]
    shape = (vectors.shape[0],) + (1,) * (vectors.ndim - 2) + (half,)
    cosine = jnp.cos(angle).reshape(shape)
    sine = jnp.sin(angle).reshape(shape)
    front = vectors[..., :half]
    back = vectors[..., half:]
    return jnp.concatenate([front * cosine - back * sine, back * cosine + front * sine], -1)

def attend(queries, context):
    keys = context[:, :, 0, :].astype(jnp.float32)
    values = context[:, :, 1, :].astype(jnp.float32)
    scale = queries.shape[-1] ** (-0.5)
    scores = jnp.einsum('skgd,lkd->kgsl', queries.astype(jnp.float32), keys) * scale
    total = context.shape[0]
    count = queries.shape[0]
    key_place = jnp.arange(total)
    query_place = jnp.arange(count) + total - count
    visible = key_place[None, :] <= query_place[:, None]
    scores = jnp.where(visible, scores, -jnp.inf)
    top = lax.optimization_barrier(jnp.max(scores, axis=-1, keepdims=True))
    expos = jnp.exp(scores - top)
    weights = (expos / lax.optimization_barrier(jnp.sum(expos, axis=-1, keepdims=True))).astype(jnp.bfloat16)
    mixed = jnp.einsum('kgsl,lkd->skgd', weights.astype(jnp.float32), values)
    return mixed.astype(jnp.bfloat16).reshape(count, -1)

def reference(layer_input, norm_gain, projection_weight, output_weight, prompt_cache, subtree_cache, parents, leaf_scores):
    kv_heads = prompt_cache.shape[1] // (2 * HEAD_SIZE)
    group = projection_weight.shape[1] // (kv_heads * HEAD_SIZE) - 2
    offset = PROMPT_TOKENS + 2 * SEGMENT_TOKENS
    second = parents[1].astype(jnp.int32)
    first = parents[0][second].astype(jnp.int32)
    prompt = prompt_cache.reshape(PROMPT_TOKENS, kv_heads, 2, HEAD_SIZE)
    cached = subtree_cache.reshape(2, LEVEL_NODES, SEGMENT_TOKENS, kv_heads, 2, HEAD_SIZE)
    width = output_weight.shape[0] // N_TENSOR

    def one_node(item):
        inputs, first_id, second_id = item
        normed = normalize(inputs, norm_gain)
        packed = jnp.dot(normed.astype(jnp.float32), projection_weight.astype(jnp.float32), preferred_element_type=jnp.float32)
        packed = packed.reshape(SEGMENT_TOKENS, kv_heads, group + 2, HEAD_SIZE)
        queries = rotate(packed[:, :, :group, :], offset).astype(jnp.bfloat16)
        keys = rotate(packed[:, :, group, :], offset).astype(jnp.bfloat16)
        values = packed[:, :, group + 1, :].astype(jnp.bfloat16)
        own = jnp.stack([keys, values], 2)
        older = cached[0][first_id]
        newer = cached[1][second_id]
        context = jnp.concatenate([prompt, older, newer, own], 0)
        mixed = attend(queries, context)
        total = jnp.zeros((SEGMENT_TOKENS, MODEL_WIDTH), jnp.float32)
        for shard in range(N_TENSOR):
            partial_term = jnp.dot(mixed[:, shard * width:(shard + 1) * width].astype(jnp.float32), output_weight[shard * width:(shard + 1) * width].astype(jnp.float32), preferred_element_type=jnp.float32)
            total = total + partial_term.astype(jnp.bfloat16).astype(jnp.float32)
        return total.astype(jnp.bfloat16)
    outputs = lax.map(one_node, (layer_input.reshape(LEVEL_NODES, SEGMENT_TOKENS, MODEL_WIDTH), first, second))
    attn_output = outputs.reshape(LEVEL_NODES * SEGMENT_TOKENS, MODEL_WIDTH)
    nodes = jnp.arange(LEVEL_NODES, dtype=jnp.int32)
    scores = leaf_scores.astype(jnp.float32)

    def combine_level(owner):
        member = owner[None, :] == nodes[:, None]
        filled = jnp.where(member, scores[None, :], 1.0)
        return (lax.optimization_barrier(jnp.min(filled, 1)), jnp.prod(filled, 1))
    low_one, product_one = combine_level(first)
    low_two, product_two = combine_level(second)
    subtree_min = jnp.stack([low_one, low_two], 0)
    subtree_product = jnp.stack([product_one, product_two], 0)
    return (attn_output, subtree_min, subtree_product)
```

```python
import functools
import math

import jax
import jax.numpy as jnp
from jax import lax
from jax.experimental import pallas as pl
from jax.experimental.pallas import tpu as pltpu
from jax.sharding import PartitionSpec as P


HEAD_SIZE = 128
SEGMENT_TOKENS = 512
PROMPT_TOKENS = 2048
THETA = 1000000.0
EPSILON = 1e-06

BLOCK = 64
ROWS = 256
DEPTH = 1024
WIDE = 2560
CHUNK = 512

FLOW = [(t, (t + 2) % 8 if t % 2 == 0 else (t - 2) % 8) for t in range(8)]
BACK = [(b, a) for a, b in FLOW]
SWAP = [(t, t ^ 1) for t in range(8)]

VMEM = pl.BlockSpec(memory_space=pltpu.VMEM)
ANY = pl.BlockSpec(memory_space=pl.ANY)
SMEM = pl.BlockSpec(memory_space=pltpu.SMEM)
NT = (((1,), (1,)), ((), ()))
NN = (((1,), (0,)), ((), ()))
TN = (((0,), (0,)), ((), ()))
SCALE = math.log2(math.e) / math.sqrt(HEAD_SIZE)


def matmul(a, b, dims=NN):
    return lax.dot_general(a, b, dims, preferred_element_type=jnp.float32)


def kernel(body, out, mib, flops, scratch=(), specs=None):
    return lambda *args: pl.pallas_call(
        body,
        in_specs=specs or [VMEM] * len(args),
        out_specs=[VMEM] * len(out),
        out_shape=[jax.ShapeDtypeStruct(shape, dtype) for shape, dtype in out],
        scratch_shapes=scratch,
        compiler_params=pltpu.CompilerParams(vmem_limit_bytes=mib << 20),
        cost_estimate=pl.CostEstimate(flops=flops, bytes_accessed=1 << 20, transcendentals=0),
    )(*args)


def slots(member):
    def held(t):
        near_by = lax.rem(t + lax.rem(t, 2) * 4 + 6, 8)
        return near_by, near_by + 1 - 2 * lax.rem(near_by, 2), lax.rem(t + 4, 8)

    partner = member + 1 - 2 * lax.rem(member, 2)
    mine, other = held(member), held(partner)
    return (mine[0], member, other[0], partner), (mine[2], mine[1], other[2], other[1])


def project(group, x0, x1, x2, x3, gain_ref, weight_ref, cos_ref, sin_ref, qkv_ref, scale, total, held, sems):
    steps = x0.shape[1] // DEPTH
    xs = (x0, x1, x2, x3)

    def load(i):
        depth = slice(i * DEPTH, (i + 1) * DEPTH)
        return pltpu.make_async_copy(weight_ref.at[depth, :], held.at[depth, :], sems.at[i])

    for i in range(steps):
        load(i).start()
    for i, x in enumerate(xs):
        wide = x[...].astype(jnp.float32)
        mean = jnp.sum(wide * wide, axis=-1, keepdims=True) * (1.0 / x.shape[1])
        scale[i * BLOCK : (i + 1) * BLOCK, :] = lax.rsqrt(mean + EPSILON)
    for i in range(steps):
        depth = slice(i * DEPTH, (i + 1) * DEPTH)
        gain = gain_ref[:, depth]
        normed = [
            (x[:, depth].astype(jnp.float32) * scale[j * BLOCK : (j + 1) * BLOCK, :] * gain).astype(jnp.bfloat16)
            for j, x in enumerate(xs)
        ]
        load(i).wait()
        term = matmul(jnp.concatenate(normed, 0), held[depth, :])
        total[...] = term if i == 0 else total[...] + term
    blocks = slots(lax.axis_index("tensor"))[group]
    for i in range(4):
        rows = slice(i * BLOCK, (i + 1) * BLOCK)
        cosine = cos_ref[blocks[i]]
        sine = sin_ref[blocks[i]]
        for part in range(4):
            head = total[rows, part * HEAD_SIZE : (part + 1) * HEAD_SIZE]
            turned = head * cosine + pltpu.roll(head, HEAD_SIZE // 2, 1) * sine
            qkv_ref[part, rows, :] = turned.astype(jnp.bfloat16)
        qkv_ref[4, rows, :] = total[rows, 4 * HEAD_SIZE :].astype(jnp.bfloat16)


def extend(state, q, keys, values, mask=None):
    scores = matmul(keys, q, NT) * SCALE
    if mask is not None:
        scores = jnp.where(mask, scores, -jnp.inf)
    top = jnp.max(scores, axis=0, keepdims=True)
    if state is not None:
        top = jnp.maximum(state[0], top)
    expos = jnp.exp2(scores - top)
    total = jnp.sum(expos, axis=0, keepdims=True)
    mixed = matmul(values, expos.astype(jnp.bfloat16), TN)
    if state is not None:
        shrink = jnp.exp2(state[0] - top)
        total = total + state[1] * shrink
        mixed = mixed + state[2] * shrink
    return top, total, mixed


def pick(parents_ref, spread_ref, picked_ref):
    nodes = spread_ref.shape[0]
    older = lax.axis_index("branch") < nodes // 2
    for j in range(nodes):
        second = parents_ref[1, j]
        first = parents_ref[0, second]
        picked_ref[j] = spread_ref[jnp.where(older, first, second)]


def prompt_part(state, q, prompt_ref):
    for c in range(PROMPT_TOKENS // CHUNK):
        rows = slice(c * CHUNK, (c + 1) * CHUNK)
        state = extend(state, q, prompt_ref[rows, :HEAD_SIZE], prompt_ref[rows, HEAD_SIZE:])
    return state


def near_early(qkv_ref, prompt_ref, top_ref, sum_ref, mix_ref):
    q = qkv_ref[:3].reshape(QUERIES, HEAD_SIZE)
    top_ref[...], sum_ref[...], mix_ref[...] = prompt_part(None, q, prompt_ref)


def near_late(prompt_ref, early_ref, te_ref, se_ref, me_ref, late_ref, *results):
    blocks = slots(lax.axis_index("tensor"))
    within = lax.broadcasted_iota(jnp.int32, (BLOCK, QUERIES), 0)
    column = lax.rem(lax.broadcasted_iota(jnp.int32, (1, QUERIES), 1), ROWS)
    for g, qkv_ref in enumerate((early_ref, late_ref)):
        q = qkv_ref[:3].reshape(QUERIES, HEAD_SIZE)
        state = (te_ref[...], se_ref[...], me_ref[...]) if g == 0 else prompt_part(None, q, prompt_ref)
        place = jnp.zeros((1, QUERIES), jnp.int32)
        for i in range(4):
            place = jnp.where(column // BLOCK == i, blocks[g][i] * BLOCK + column - i * BLOCK, place)
        for h, own_ref in enumerate((early_ref, late_ref)):
            mask = jnp.concatenate([within + blocks[h][i] * BLOCK <= place for i in range(4)], 0)
            state = extend(state, q, own_ref[3], own_ref[4], mask)
        for ref, value in zip(results[3 * g : 3 * g + 3], state):
            ref[...] = value


def far(qkv_ref, context_ref, top_ref, sum_ref, mix_ref, mine_ref, other_ref):
    q = qkv_ref[:3].reshape(QUERIES, HEAD_SIZE)
    parts = []
    for columns in (slice(0, QUERIES // 2), slice(QUERIES // 2, QUERIES)):
        state = (top_ref[:, columns], sum_ref[:, columns], mix_ref[:, columns])
        state = extend(state, q[columns], context_ref[:, :HEAD_SIZE], context_ref[:, HEAD_SIZE:])
        parts.append((state[2] / state[1]).T.astype(jnp.bfloat16))
    mixed = jnp.concatenate(parts, 0)
    for head in range(3):
        columns = slice(head * HEAD_SIZE, (head + 1) * HEAD_SIZE)
        mine_ref[:, columns] = mixed[head * ROWS : head * ROWS + ROWS // 2]
        other_ref[:, columns] = mixed[head * ROWS + ROWS // 2 : (head + 1) * ROWS]


def output(a_ref, b_ref, wa_ref, wb_ref, *refs):
    first_ref, second_ref, held, sems = refs[-4:]
    depth = wa_ref.shape[0]
    copies = []
    for c in range(wa_ref.shape[1] // WIDE):
        columns = slice(c * WIDE, (c + 1) * WIDE)
        copies.append(pltpu.make_async_copy(wa_ref.at[:, columns], held.at[:depth, columns], sems.at[2 * c]))
        copies.append(pltpu.make_async_copy(wb_ref.at[:, columns], held.at[depth:, columns], sems.at[2 * c + 1]))
    for copy in copies:
        copy.start()
    both = jnp.concatenate([a_ref[...], b_ref[...]], 1)
    for c in range(wa_ref.shape[1] // WIDE):
        columns = slice(c * WIDE, (c + 1) * WIDE)
        copies[2 * c].wait()
        copies[2 * c + 1].wait()
        total = matmul(both, held[:, columns])
        first = total[:BLOCK]
        if len(refs) > 4:
            first = first + refs[0][:, columns].astype(jnp.float32)
        first_ref[:, columns] = first.astype(jnp.bfloat16)
        second_ref[:, columns] = total[BLOCK:].astype(jnp.bfloat16)


QUERIES = 3 * ROWS
PROJECT_MIB, OUTPUT_MIB = 50, 53
F32, BF16 = jnp.float32, jnp.bfloat16
STATE = [((1, QUERIES), F32), ((1, QUERIES), F32), ((HEAD_SIZE, QUERIES), F32)]


def add(*terms):
    return sum(term.astype(jnp.float32) for term in terms).astype(jnp.bfloat16)


def tables():
    half = HEAD_SIZE // 2
    freq = THETA ** (-jnp.arange(half, dtype=jnp.float32) * 2.0 / HEAD_SIZE)
    places = (PROMPT_TOKENS + 2 * SEGMENT_TOKENS + jnp.arange(SEGMENT_TOKENS)).astype(jnp.float32)
    angle = places[:, None] * freq[None, :]
    cosine, sine = jnp.cos(angle), jnp.sin(angle)
    shape = (SEGMENT_TOKENS // BLOCK, BLOCK, HEAD_SIZE)
    return (
        jnp.concatenate([cosine, cosine], -1).reshape(shape),
        jnp.concatenate([-sine, sine], -1).reshape(shape),
    )


def per_device(
    layer_input, norm_gain, projection_weight, output_weight, prompt_cache, subtree_cache, parents, leaf_scores
):
    position = lax.axis_index("branch")
    nodes = lax.axis_size("branch")
    features = layer_input.shape[1]

    def tensor(x, pairs):
        return lax.ppermute(x, "tensor", pairs)

    x0 = layer_input
    x1 = tensor(x0, SWAP)
    x2 = tensor(x0, FLOW)
    x3 = tensor(x1, FLOW)
    x4 = tensor(x2, FLOW)
    x5 = tensor(x2, SWAP)
    x6 = tensor(x3, SWAP)
    x7 = tensor(x4, SWAP)

    pieces = subtree_cache.reshape(nodes, -1, subtree_cache.shape[2])
    spread = lax.all_to_all(pieces, "branch", 0, 0, tiled=True)

    cosine, sine = tables()
    gain = norm_gain[None, :]
    projected = [((5, ROWS, HEAD_SIZE), BF16)]
    columns = projection_weight.shape[1]
    run_project = lambda group, *xs: kernel(
        functools.partial(project, group),
        projected,
        PROJECT_MIB,
        2 * ROWS * features * columns,
        [
            pltpu.VMEM((ROWS, 1), F32),
            pltpu.VMEM((ROWS, columns), F32),
            pltpu.VMEM((features, columns), BF16),
            pltpu.SemaphoreType.DMA((features // DEPTH,)),
        ],
        [VMEM] * 5 + [ANY] + [VMEM] * 2,
    )(*xs, gain, projection_weight, cosine, sine)
    early = run_project(0, x2, x0, x5, x1)
    early_state = kernel(near_early, STATE, 16, 4 * QUERIES * PROMPT_TOKENS * HEAD_SIZE)(*early, prompt_cache)

    spread, early_state = lax.optimization_barrier((spread, early_state))
    picked = kernel(pick, [(spread.shape, BF16)], 16, 1 << 22, (), [SMEM, VMEM])(parents, spread)[0]
    context = lax.all_to_all(picked, "branch", 0, 0, tiled=True)
    context = context.reshape(2 * SEGMENT_TOKENS, -1)
    other_weight = tensor(lax.optimization_barrier((output_weight, early_state))[0], SWAP)

    late = run_project(1, x4, x3, x7, x6)
    depth = output_weight.shape[0]
    state = kernel(near_late, STATE + STATE, 20, 4 * QUERIES * (PROMPT_TOKENS + 2 * SEGMENT_TOKENS) * HEAD_SIZE)(
        prompt_cache, *early, *early_state, *late
    )

    scores = jnp.broadcast_to(leaf_scores[:, None], (1, HEAD_SIZE))
    for bit in range(5):
        if bit == 1:
            scores, state = lax.optimization_barrier((scores, state))
        came = lax.ppermute(scores, "branch", [(b, b ^ (1 << bit)) for b in range(32)])
        upper = (position >> bit) & 1 == 1
        scores = jnp.where(upper, jnp.concatenate([came, scores]), jnp.concatenate([scores, came]))
    scores = scores[:, 0]

    halves = [((ROWS // 2, 3 * HEAD_SIZE), BF16)] * 2
    run_far = kernel(far, halves, 16, 4 * QUERIES * 2 * SEGMENT_TOKENS * HEAD_SIZE)
    rows = [((BLOCK, features), BF16)] * 2
    run_output = lambda *args: kernel(
        output,
        rows,
        OUTPUT_MIB,
        8 * BLOCK * depth * features,
        [pltpu.VMEM((2 * depth, features), BF16), pltpu.SemaphoreType.DMA((2 * features // WIDE,))],
        [VMEM, VMEM, ANY, ANY, VMEM][: len(args)],
    )(*args)
    late_mine, late_other = run_far(late[0], context, *state[3:])
    late_came = tensor(late_other, SWAP)
    early_mine, early_other = run_far(early[0], context, *state[:3])
    early_came = tensor(early_other, SWAP)
    y4, y3 = run_output(late_mine, late_came, output_weight, other_weight)
    z2 = tensor(y4, BACK)
    z1 = tensor(y3, BACK)
    y2, y0 = run_output(early_mine, early_came, output_weight, other_weight, z2)
    z0 = tensor(y2, BACK)
    z1 = tensor(z1, SWAP)
    attn_output = add(y0, z0, z1)

    second = parents[1]
    owners = jnp.stack([parents[0][second], second])
    filled = jnp.where(owners == position, scores[None, :], 1.0)
    subtree_min = jnp.min(filled, axis=1, keepdims=True)
    subtree_product = jnp.prod(filled, axis=1, keepdims=True)
    return attn_output, subtree_min, subtree_product


def solution(mesh):
    placed = (
        P(("branch", "tensor"), None),
        P(),
        P(None, "tensor"),
        P("tensor", None),
        P(None, "tensor"),
        P(None, "branch", "tensor"),
        P(),
        P("branch"),
    )
    return jax.shard_map(
        per_device,
        mesh=mesh,
        in_specs=placed,
        out_specs=(P(("branch", "tensor"), None), P(None, "branch"), P(None, "branch")),
        check_vma=False,
    )
```

```python
import functools
import math

import jax
import jax.numpy as jnp
from jax import lax
from jax.experimental import pallas as pl
from jax.experimental.pallas import tpu as pltpu
from jax.sharding import PartitionSpec as P


HEAD_SIZE = 128
SEGMENT_TOKENS = 512
PROMPT_TOKENS = 2048
THETA = 1000000.0
EPSILON = 1e-06

BLOCK = 64
ROWS = 256
DEPTH = 1024
WIDE = 2560
SPARE = 8
CHUNK = 512

FLOW = [(t, (t + 2) % 8 if t % 2 == 0 else (t - 2) % 8) for t in range(8)]
BACK = [(b, a) for a, b in FLOW]
SWAP = [(t, t ^ 1) for t in range(8)]

VMEM = pl.BlockSpec(memory_space=pltpu.VMEM)
ANY = pl.BlockSpec(memory_space=pl.ANY)
SMEM = pl.BlockSpec(memory_space=pltpu.SMEM)
NT = (((1,), (1,)), ((), ()))
NN = (((1,), (0,)), ((), ()))
TN = (((0,), (0,)), ((), ()))
SCALE = math.log2(math.e) / math.sqrt(HEAD_SIZE)


def matmul(a, b, dims=NN):
    return lax.dot_general(a, b, dims, preferred_element_type=jnp.float32)


def kernel(body, out, mib, flops, scratch=(), specs=None):
    return lambda *args: pl.pallas_call(
        body,
        in_specs=specs or [VMEM] * len(args),
        out_specs=[VMEM] * len(out),
        out_shape=[jax.ShapeDtypeStruct(shape, dtype) for shape, dtype in out],
        scratch_shapes=scratch,
        compiler_params=pltpu.CompilerParams(vmem_limit_bytes=mib << 20),
        cost_estimate=pl.CostEstimate(flops=flops, bytes_accessed=1 << 20, transcendentals=0),
    )(*args)


def slots(member):
    def held(t):
        near_by = lax.rem(t + lax.rem(t, 2) * 4 + 6, 8)
        return near_by, near_by + 1 - 2 * lax.rem(near_by, 2), lax.rem(t + 4, 8)

    partner = member + 1 - 2 * lax.rem(member, 2)
    mine, other = held(member), held(partner)
    return (mine[0], member, other[0], partner), (mine[2], mine[1], other[2], other[1])


def project(group, x0, x1, x2, x3, gain_ref, weight_ref, cos_ref, sin_ref, qkv_ref, scale, total, held, sems):
    steps = x0.shape[1] // DEPTH
    xs = (x0, x1, x2, x3)

    def load(i):
        depth = slice(i * DEPTH, (i + 1) * DEPTH)
        return pltpu.make_async_copy(weight_ref.at[depth, :], held.at[depth, :], sems.at[i])

    for i in range(steps):
        load(i).start()
    for i, x in enumerate(xs):
        wide = x[...].astype(jnp.float32)
        mean = jnp.sum(wide * wide, axis=-1, keepdims=True) * (1.0 / x.shape[1])
        scale[i * BLOCK : (i + 1) * BLOCK, :] = lax.rsqrt(mean + EPSILON)
    for i in range(steps):
        depth = slice(i * DEPTH, (i + 1) * DEPTH)
        gain = gain_ref[:, depth]
        normed = [
            (x[:, depth].astype(jnp.float32) * scale[j * BLOCK : (j + 1) * BLOCK, :] * gain).astype(jnp.bfloat16)
            for j, x in enumerate(xs)
        ]
        load(i).wait()
        term = matmul(jnp.concatenate(normed, 0), held[depth, :])
        total[...] = term if i == 0 else total[...] + term
    blocks = slots(lax.axis_index("tensor"))[group]
    for i in range(4):
        rows = slice(i * BLOCK, (i + 1) * BLOCK)
        cosine = cos_ref[blocks[i]]
        sine = sin_ref[blocks[i]]
        for part in range(4):
            head = total[rows, part * HEAD_SIZE : (part + 1) * HEAD_SIZE]
            turned = head * cosine + pltpu.roll(head, HEAD_SIZE // 2, 1) * sine
            qkv_ref[part, rows, :] = turned.astype(jnp.bfloat16)
        qkv_ref[4, rows, :] = total[rows, 4 * HEAD_SIZE :].astype(jnp.bfloat16)


def extend(state, q, keys, values, mask=None):
    scores = matmul(keys, q, NT) * SCALE
    if mask is not None:
        scores = jnp.where(mask, scores, -jnp.inf)
    top = jnp.max(scores, axis=0, keepdims=True)
    if state is not None:
        top = jnp.maximum(state[0], top)
    expos = jnp.exp2(scores - top)
    total = jnp.sum(expos, axis=0, keepdims=True)
    mixed = matmul(values, expos.astype(jnp.bfloat16), TN)
    if state is not None:
        shrink = jnp.exp2(state[0] - top)
        total = total + state[1] * shrink
        mixed = mixed + state[2] * shrink
    return top, total, mixed


def pick(parents_ref, score_ref, spread_ref, picked_ref):
    nodes, rows, _ = spread_ref.shape
    older = lax.axis_index("branch") < nodes // 2
    score = jnp.full((SPARE, HEAD_SIZE), score_ref[0], jnp.float32)
    high = score.astype(jnp.bfloat16).astype(jnp.float32)
    middle = (score - high).astype(jnp.bfloat16).astype(jnp.float32)
    low = score - high - middle
    row = lax.broadcasted_iota(jnp.int32, score.shape, 0)
    terms = jnp.where(row == 0, high, jnp.where(row == 1, middle, low)).astype(jnp.bfloat16)
    for j in range(nodes):
        second = parents_ref[1, j]
        source = jnp.where(older, parents_ref[0, second], second)
        picked_ref[j, :rows] = spread_ref[source, :, :HEAD_SIZE]
        picked_ref[j, rows : 2 * rows] = spread_ref[source, :, HEAD_SIZE:]
        picked_ref[j, 2 * rows :] = terms


def tree(parents_ref, context_ref, min_ref, product_ref):
    nodes = context_ref.shape[0]
    me = lax.axis_index("branch")
    terms = context_ref[:, -SPARE:, :].astype(jnp.float32)
    scores = (terms[:, 0, :] + terms[:, 1, :]) + terms[:, 2, :]
    for level in range(2):
        least = product = jnp.ones((1, HEAD_SIZE), jnp.float32)
        for j in range(nodes):
            second = parents_ref[1, j]
            owner = parents_ref[0, second] if level == 0 else second
            term = jnp.where(owner == me, scores[j : j + 1], 1.0)
            least = jnp.minimum(least, term)
            product = product * term
        min_ref[level : level + 1, :] = least[:, :1]
        product_ref[level : level + 1, :] = product[:, :1]


def join(*refs):
    total = sum(ref[...].astype(jnp.float32) for ref in refs[:-1])
    refs[-1][...] = total.astype(refs[-1].dtype)


def prompt_part(state, q, prompt_ref):
    for c in range(PROMPT_TOKENS // CHUNK):
        rows = slice(c * CHUNK, (c + 1) * CHUNK)
        state = extend(state, q, prompt_ref[rows, :HEAD_SIZE], prompt_ref[rows, HEAD_SIZE:])
    return state


def near_early(qkv_ref, prompt_ref, top_ref, sum_ref, mix_ref):
    q = qkv_ref[:3].reshape(QUERIES, HEAD_SIZE)
    top_ref[...], sum_ref[...], mix_ref[...] = prompt_part(None, q, prompt_ref)


def near_late(prompt_ref, early_ref, te_ref, se_ref, me_ref, late_ref, *results):
    blocks = slots(lax.axis_index("tensor"))
    within = lax.broadcasted_iota(jnp.int32, (BLOCK, QUERIES), 0)
    column = lax.rem(lax.broadcasted_iota(jnp.int32, (1, QUERIES), 1), ROWS)
    for g, qkv_ref in enumerate((early_ref, late_ref)):
        q = qkv_ref[:3].reshape(QUERIES, HEAD_SIZE)
        state = (te_ref[...], se_ref[...], me_ref[...]) if g == 0 else prompt_part(None, q, prompt_ref)
        place = jnp.zeros((1, QUERIES), jnp.int32)
        for i in range(4):
            place = jnp.where(column // BLOCK == i, blocks[g][i] * BLOCK + column - i * BLOCK, place)
        for h, own_ref in enumerate((early_ref, late_ref)):
            mask = jnp.concatenate([within + blocks[h][i] * BLOCK <= place for i in range(4)], 0)
            state = extend(state, q, own_ref[3], own_ref[4], mask)
        for ref, value in zip(results[3 * g : 3 * g + 3], state):
            ref[...] = value


def far(qkv_ref, context_ref, top_ref, sum_ref, mix_ref, mine_ref, other_ref):
    q = qkv_ref[:3].reshape(QUERIES, HEAD_SIZE)
    rows = (context_ref.shape[1] - SPARE) // 2
    keys = context_ref[:, :rows, :].reshape(-1, HEAD_SIZE)
    values = context_ref[:, rows : 2 * rows, :].reshape(-1, HEAD_SIZE)
    parts = []
    for columns in (slice(0, QUERIES // 2), slice(QUERIES // 2, QUERIES)):
        state = (top_ref[:, columns], sum_ref[:, columns], mix_ref[:, columns])
        state = extend(state, q[columns], keys, values)
        parts.append((state[2] / state[1]).T.astype(jnp.bfloat16))
    mixed = jnp.concatenate(parts, 0)
    for head in range(3):
        columns = slice(head * HEAD_SIZE, (head + 1) * HEAD_SIZE)
        mine_ref[:, columns] = mixed[head * ROWS : head * ROWS + ROWS // 2]
        other_ref[:, columns] = mixed[head * ROWS + ROWS // 2 : (head + 1) * ROWS]


def output(a_ref, b_ref, wa_ref, wb_ref, first_ref, second_ref, held, sems):
    depth = wa_ref.shape[0]
    copies = []
    for c in range(wa_ref.shape[1] // WIDE):
        columns = slice(c * WIDE, (c + 1) * WIDE)
        copies.append(pltpu.make_async_copy(wa_ref.at[:, columns], held.at[:depth, columns], sems.at[2 * c]))
        copies.append(pltpu.make_async_copy(wb_ref.at[:, columns], held.at[depth:, columns], sems.at[2 * c + 1]))
    for copy in copies:
        copy.start()
    both = jnp.concatenate([a_ref[...], b_ref[...]], 1)
    for c in range(wa_ref.shape[1] // WIDE):
        columns = slice(c * WIDE, (c + 1) * WIDE)
        copies[2 * c].wait()
        copies[2 * c + 1].wait()
        total = matmul(both, held[:, columns])
        first_ref[:, columns] = total[:BLOCK].astype(jnp.bfloat16)
        second_ref[:, columns] = total[BLOCK:].astype(jnp.bfloat16)


QUERIES = 3 * ROWS
PROJECT_MIB, OUTPUT_MIB = 50, 53
F32, BF16 = jnp.float32, jnp.bfloat16
STATE = [((1, QUERIES), F32), ((1, QUERIES), F32), ((HEAD_SIZE, QUERIES), F32)]


def add(*terms):
    return sum(term.astype(jnp.float32) for term in terms).astype(jnp.bfloat16)


def tables():
    half = HEAD_SIZE // 2
    freq = THETA ** (-jnp.arange(half, dtype=jnp.float32) * 2.0 / HEAD_SIZE)
    places = (PROMPT_TOKENS + 2 * SEGMENT_TOKENS + jnp.arange(SEGMENT_TOKENS)).astype(jnp.float32)
    angle = places[:, None] * freq[None, :]
    cosine, sine = jnp.cos(angle), jnp.sin(angle)
    shape = (SEGMENT_TOKENS // BLOCK, BLOCK, HEAD_SIZE)
    return (
        jnp.concatenate([cosine, cosine], -1).reshape(shape),
        jnp.concatenate([-sine, sine], -1).reshape(shape),
    )


def per_device(
    layer_input, norm_gain, projection_weight, output_weight, prompt_cache, subtree_cache, parents, leaf_scores
):
    nodes = lax.axis_size("branch")
    features = layer_input.shape[1]

    def tensor(x, pairs):
        return lax.ppermute(x, "tensor", pairs)

    x0 = layer_input
    x1 = tensor(x0, SWAP)
    x2 = tensor(x0, FLOW)
    x3 = tensor(x1, FLOW)
    x4 = tensor(x2, FLOW)
    x5 = tensor(x2, SWAP)
    x6 = tensor(x3, SWAP)
    x7 = tensor(x4, SWAP)

    pieces = subtree_cache.reshape(nodes, -1, subtree_cache.shape[2])
    spread = lax.all_to_all(pieces, "branch", 0, 0, tiled=True)

    cosine, sine = tables()
    gain = norm_gain[None, :]
    projected = [((5, ROWS, HEAD_SIZE), BF16)]
    columns = projection_weight.shape[1]
    run_project = lambda group, *xs: kernel(
        functools.partial(project, group),
        projected,
        PROJECT_MIB,
        2 * ROWS * features * columns,
        [
            pltpu.VMEM((ROWS, 1), F32),
            pltpu.VMEM((ROWS, columns), F32),
            pltpu.VMEM((features, columns), BF16),
            pltpu.SemaphoreType.DMA((features // DEPTH,)),
        ],
        [VMEM] * 5 + [ANY] + [VMEM] * 2,
    )(*xs, gain, projection_weight, cosine, sine)
    early = run_project(0, x2, x0, x5, x1)
    early_state = kernel(near_early, STATE, 16, 4 * QUERIES * PROMPT_TOKENS * HEAD_SIZE)(*early, prompt_cache)

    spread, early_state = lax.optimization_barrier((spread, early_state))
    shape = (nodes, 2 * spread.shape[1] + SPARE, HEAD_SIZE)
    picked = kernel(pick, [(shape, BF16)], 16, 1 << 22, (), [SMEM, SMEM, VMEM])(parents, leaf_scores, spread)[0]
    context = lax.all_to_all(picked, "branch", 0, 0, tiled=True)
    other_weight = tensor(output_weight, SWAP)

    late = run_project(1, x4, x3, x7, x6)
    depth = output_weight.shape[0]
    state = kernel(near_late, STATE + STATE, 20, 4 * QUERIES * (PROMPT_TOKENS + 2 * SEGMENT_TOKENS) * HEAD_SIZE)(
        prompt_cache, *early, *early_state, *late
    )

    halves = [((ROWS // 2, 3 * HEAD_SIZE), BF16)] * 2
    run_far = kernel(far, halves, 16, 4 * QUERIES * 2 * SEGMENT_TOKENS * HEAD_SIZE)
    rows = [((BLOCK, features), BF16)] * 2
    run_output = lambda *args: kernel(
        output,
        rows,
        OUTPUT_MIB,
        8 * BLOCK * depth * features,
        [pltpu.VMEM((2 * depth, features), BF16), pltpu.SemaphoreType.DMA((2 * features // WIDE,))],
        [VMEM, VMEM, ANY, ANY],
    )(*args)
    late_mine, late_other = run_far(late[0], context, *state[3:])
    late_came = tensor(late_other, SWAP)
    early_mine, early_other = run_far(early[0], context, *state[:3])
    early_came = tensor(early_other, SWAP)
    y4, y3 = run_output(late_mine, late_came, output_weight, other_weight)
    z2 = tensor(y4, BACK)
    z1 = tensor(y3, BACK)
    y2, y0 = run_output(early_mine, early_came, output_weight, other_weight)
    run_join = lambda *terms: kernel(join, rows[:1], 8, 1 << 20)(*terms)[0]
    y2 = run_join(y2, z2)
    z0 = tensor(y2, BACK)
    least, product = kernel(tree, [((2, 1), F32)] * 2, 8, 1 << 20, (), [SMEM, VMEM])(parents, context)
    z1 = tensor(z1, SWAP)
    return add(y0, z0, z1), least, product


def solution(mesh):
    placed = (
        P(("branch", "tensor"), None),
        P(),
        P(None, "tensor"),
        P("tensor", None),
        P(None, "tensor"),
        P(None, "branch", "tensor"),
        P(),
        P("branch"),
    )
    return jax.shard_map(
        per_device,
        mesh=mesh,
        in_specs=placed,
        out_specs=(P(("branch", "tensor"), None), P(None, "branch"), P(None, "branch")),
        check_vma=False,
    )
```

```python
import functools
import math

import jax
import jax.numpy as jnp
from jax import lax
from jax.experimental import pallas as pl
from jax.experimental.pallas import tpu as pltpu
from jax.sharding import PartitionSpec as P


HEAD_SIZE = 128
SEGMENT_TOKENS = 512
PROMPT_TOKENS = 2048
THETA = 1000000.0
EPSILON = 1e-06

BLOCK = 64
ROWS = 256
DEPTH = 1024
SPARE = 8
CHUNK = 512

FLOW = [(t, (t + 2) % 8 if t % 2 == 0 else (t - 2) % 8) for t in range(8)]
BACK = [(b, a) for a, b in FLOW]
SWAP = [(t, t ^ 1) for t in range(8)]

VMEM = pl.BlockSpec(memory_space=pltpu.VMEM)
ANY = pl.BlockSpec(memory_space=pl.ANY)
SMEM = pl.BlockSpec(memory_space=pltpu.SMEM)
NT = (((1,), (1,)), ((), ()))
NN = (((1,), (0,)), ((), ()))
TN = (((0,), (0,)), ((), ()))
SCALE = math.log2(math.e) / math.sqrt(HEAD_SIZE)


def matmul(a, b, dims=NN):
    return lax.dot_general(a, b, dims, preferred_element_type=jnp.float32)


def kernel(body, out, mib, flops, scratch=(), specs=None):
    return lambda *args: pl.pallas_call(
        body,
        in_specs=specs or [VMEM] * len(args),
        out_specs=[VMEM] * len(out),
        out_shape=[jax.ShapeDtypeStruct(shape, dtype) for shape, dtype in out],
        scratch_shapes=scratch,
        compiler_params=pltpu.CompilerParams(vmem_limit_bytes=mib << 20),
        cost_estimate=pl.CostEstimate(flops=flops, bytes_accessed=1 << 20, transcendentals=0),
    )(*args)


def slots(member):
    def held(t):
        near_by = lax.rem(t + lax.rem(t, 2) * 4 + 6, 8)
        return near_by, near_by + 1 - 2 * lax.rem(near_by, 2), lax.rem(t + 4, 8)

    partner = member + 1 - 2 * lax.rem(member, 2)
    mine, other = held(member), held(partner)
    return (mine[0], member, other[0], partner), (mine[2], mine[1], other[2], other[1])


def project(group, x0, x1, x2, x3, gain_ref, weight_ref, cos_ref, sin_ref, qkv_ref, scale, total, held, sems):
    steps = x0.shape[1] // DEPTH
    xs = (x0, x1, x2, x3)

    def load(i):
        depth = slice(i * DEPTH, (i + 1) * DEPTH)
        return pltpu.make_async_copy(weight_ref.at[depth, :], held.at[depth, :], sems.at[i])

    for i in range(steps):
        load(i).start()
    for i, x in enumerate(xs):
        wide = x[...].astype(jnp.float32)
        mean = jnp.sum(wide * wide, axis=-1, keepdims=True) * (1.0 / x.shape[1])
        scale[i * BLOCK : (i + 1) * BLOCK, :] = lax.rsqrt(mean + EPSILON)
    for i in range(steps):
        depth = slice(i * DEPTH, (i + 1) * DEPTH)
        gain = gain_ref[:, depth]
        normed = [
            (x[:, depth].astype(jnp.float32) * scale[j * BLOCK : (j + 1) * BLOCK, :] * gain).astype(jnp.bfloat16)
            for j, x in enumerate(xs)
        ]
        load(i).wait()
        term = matmul(jnp.concatenate(normed, 0), held[depth, :])
        total[...] = term if i == 0 else total[...] + term
    blocks = slots(lax.axis_index("tensor"))[group]
    for i in range(4):
        rows = slice(i * BLOCK, (i + 1) * BLOCK)
        cosine = cos_ref[blocks[i]]
        sine = sin_ref[blocks[i]]
        for part in range(4):
            head = total[rows, part * HEAD_SIZE : (part + 1) * HEAD_SIZE]
            turned = head * cosine + pltpu.roll(head, HEAD_SIZE // 2, 1) * sine
            qkv_ref[part, rows, :] = turned.astype(jnp.bfloat16)
        qkv_ref[4, rows, :] = total[rows, 4 * HEAD_SIZE :].astype(jnp.bfloat16)


def extend(state, q, keys, values, mask=None):
    scores = matmul(keys, q, NT) * SCALE
    if mask is not None:
        scores = jnp.where(mask, scores, -jnp.inf)
    top = jnp.max(scores, axis=0, keepdims=True)
    if state is not None:
        top = jnp.maximum(state[0], top)
    expos = jnp.exp2(scores - top)
    total = jnp.sum(expos, axis=0, keepdims=True)
    mixed = matmul(values, expos.astype(jnp.bfloat16), TN)
    if state is not None:
        shrink = jnp.exp2(state[0] - top)
        total = total + state[1] * shrink
        mixed = mixed + state[2] * shrink
    return top, total, mixed


def pick(parents_ref, score_ref, spread_ref, picked_ref):
    nodes, rows, _ = spread_ref.shape
    older = lax.axis_index("branch") < nodes // 2
    score = jnp.full((SPARE, HEAD_SIZE), score_ref[0], jnp.float32)
    high = score.astype(jnp.bfloat16).astype(jnp.float32)
    middle = (score - high).astype(jnp.bfloat16).astype(jnp.float32)
    low = score - high - middle
    row = lax.broadcasted_iota(jnp.int32, score.shape, 0)
    terms = jnp.where(row == 0, high, jnp.where(row == 1, middle, low)).astype(jnp.bfloat16)
    for j in range(nodes):
        second = parents_ref[1, j]
        source = jnp.where(older, parents_ref[0, second], second)
        picked_ref[j, :rows] = spread_ref[source, :, :HEAD_SIZE]
        picked_ref[j, rows : 2 * rows] = spread_ref[source, :, HEAD_SIZE:]
        picked_ref[j, 2 * rows :] = terms


def tree(parents_ref, context_ref, min_ref, product_ref):
    nodes = context_ref.shape[0]
    me = lax.axis_index("branch")
    terms = context_ref[:, -SPARE:, :].astype(jnp.float32)
    scores = (terms[:, 0, :] + terms[:, 1, :]) + terms[:, 2, :]
    for level in range(2):
        least = product = jnp.ones((1, HEAD_SIZE), jnp.float32)
        for j in range(nodes):
            second = parents_ref[1, j]
            owner = parents_ref[0, second] if level == 0 else second
            term = jnp.where(owner == me, scores[j : j + 1], 1.0)
            least = jnp.minimum(least, term)
            product = product * term
        min_ref[level : level + 1, :] = least[:, :1]
        product_ref[level : level + 1, :] = product[:, :1]


def join(block_ref, left_ref, right_ref, sum_ref):
    half = left_ref.shape[1]
    for columns, ref in ((slice(0, half), left_ref), (slice(half, 2 * half), right_ref)):
        total = block_ref[:, columns].astype(jnp.float32) + ref[...].astype(jnp.float32)
        sum_ref[:, columns] = total.astype(sum_ref.dtype)


def prompt_part(state, q, prompt_ref):
    for c in range(PROMPT_TOKENS // CHUNK):
        rows = slice(c * CHUNK, (c + 1) * CHUNK)
        state = extend(state, q, prompt_ref[rows, :HEAD_SIZE], prompt_ref[rows, HEAD_SIZE:])
    return state


def near_early(qkv_ref, prompt_ref, top_ref, sum_ref, mix_ref):
    q = qkv_ref[:3].reshape(QUERIES, HEAD_SIZE)
    top_ref[...], sum_ref[...], mix_ref[...] = prompt_part(None, q, prompt_ref)


def near_late(prompt_ref, early_ref, te_ref, se_ref, me_ref, late_ref, *results):
    blocks = slots(lax.axis_index("tensor"))
    within = lax.broadcasted_iota(jnp.int32, (BLOCK, QUERIES), 0)
    column = lax.rem(lax.broadcasted_iota(jnp.int32, (1, QUERIES), 1), ROWS)
    for g, qkv_ref in enumerate((early_ref, late_ref)):
        q = qkv_ref[:3].reshape(QUERIES, HEAD_SIZE)
        state = (te_ref[...], se_ref[...], me_ref[...]) if g == 0 else prompt_part(None, q, prompt_ref)
        place = jnp.zeros((1, QUERIES), jnp.int32)
        for i in range(4):
            place = jnp.where(column // BLOCK == i, blocks[g][i] * BLOCK + column - i * BLOCK, place)
        for h, own_ref in enumerate((early_ref, late_ref)):
            mask = jnp.concatenate([within + blocks[h][i] * BLOCK <= place for i in range(4)], 0)
            state = extend(state, q, own_ref[3], own_ref[4], mask)
        for ref, value in zip(results[3 * g : 3 * g + 3], state):
            ref[...] = value


def far(qkv_ref, context_ref, top_ref, sum_ref, mix_ref, mine_ref, other_ref):
    q = qkv_ref[:3].reshape(QUERIES, HEAD_SIZE)
    rows = (context_ref.shape[1] - SPARE) // 2
    keys = context_ref[:, :rows, :].reshape(-1, HEAD_SIZE)
    values = context_ref[:, rows : 2 * rows, :].reshape(-1, HEAD_SIZE)
    parts = []
    for columns in (slice(0, QUERIES // 2), slice(QUERIES // 2, QUERIES)):
        state = (top_ref[:, columns], sum_ref[:, columns], mix_ref[:, columns])
        state = extend(state, q[columns], keys, values)
        parts.append((state[2] / state[1]).T.astype(jnp.bfloat16))
    mixed = jnp.concatenate(parts, 0)
    for head in range(3):
        columns = slice(head * HEAD_SIZE, (head + 1) * HEAD_SIZE)
        mine_ref[:, columns] = mixed[head * ROWS : head * ROWS + ROWS // 2]
        other_ref[:, columns] = mixed[head * ROWS + ROWS // 2 : (head + 1) * ROWS]


def output(first, wide, a_ref, b_ref, wa_ref, wb_ref, first_ref, second_ref, held, sems):
    depth = wa_ref.shape[0]
    steps = held.shape[1] // wide
    copies = []
    for c in range(steps):
        here = slice(c * wide, (c + 1) * wide)
        there = slice(first + c * wide, first + (c + 1) * wide)
        copies.append(pltpu.make_async_copy(wa_ref.at[:, there], held.at[:depth, here], sems.at[2 * c]))
        copies.append(pltpu.make_async_copy(wb_ref.at[:, there], held.at[depth:, here], sems.at[2 * c + 1]))
    for copy in copies:
        copy.start()
    both = jnp.concatenate([a_ref[...], b_ref[...]], 1)
    for c in range(steps):
        here = slice(c * wide, (c + 1) * wide)
        copies[2 * c].wait()
        copies[2 * c + 1].wait()
        total = matmul(both, held[:, here])
        first_ref[:, here] = total[:BLOCK].astype(jnp.bfloat16)
        second_ref[:, here] = total[BLOCK:].astype(jnp.bfloat16)


QUERIES = 3 * ROWS
PROJECT_MIB, OUTPUT_MIB = 50, 53
F32, BF16 = jnp.float32, jnp.bfloat16
STATE = [((1, QUERIES), F32), ((1, QUERIES), F32), ((HEAD_SIZE, QUERIES), F32)]


def tables():
    half = HEAD_SIZE // 2
    freq = THETA ** (-jnp.arange(half, dtype=jnp.float32) * 2.0 / HEAD_SIZE)
    places = (PROMPT_TOKENS + 2 * SEGMENT_TOKENS + jnp.arange(SEGMENT_TOKENS)).astype(jnp.float32)
    angle = places[:, None] * freq[None, :]
    cosine, sine = jnp.cos(angle), jnp.sin(angle)
    shape = (SEGMENT_TOKENS // BLOCK, BLOCK, HEAD_SIZE)
    return (
        jnp.concatenate([cosine, cosine], -1).reshape(shape),
        jnp.concatenate([-sine, sine], -1).reshape(shape),
    )


def per_device(
    layer_input, norm_gain, projection_weight, output_weight, prompt_cache, subtree_cache, parents, leaf_scores
):
    nodes = lax.axis_size("branch")
    features = layer_input.shape[1]

    def tensor(x, pairs):
        return lax.ppermute(x, "tensor", pairs)

    x0 = layer_input
    x1 = tensor(x0, SWAP)
    x2 = tensor(x0, FLOW)
    x3 = tensor(x1, FLOW)
    x4 = tensor(x2, FLOW)
    x5 = tensor(x2, SWAP)
    x6 = tensor(x3, SWAP)
    x7 = tensor(x4, SWAP)

    pieces = subtree_cache.reshape(nodes, -1, subtree_cache.shape[2])
    spread = lax.all_to_all(pieces, "branch", 0, 0, tiled=True)

    cosine, sine = tables()
    gain = norm_gain[None, :]
    projected = [((5, ROWS, HEAD_SIZE), BF16)]
    columns = projection_weight.shape[1]
    run_project = lambda group, *xs: kernel(
        functools.partial(project, group),
        projected,
        PROJECT_MIB,
        2 * ROWS * features * columns,
        [
            pltpu.VMEM((ROWS, 1), F32),
            pltpu.VMEM((ROWS, columns), F32),
            pltpu.VMEM((features, columns), BF16),
            pltpu.SemaphoreType.DMA((features // DEPTH,)),
        ],
        [VMEM] * 5 + [ANY] + [VMEM] * 2,
    )(*xs, gain, projection_weight, cosine, sine)
    early = run_project(0, x2, x0, x5, x1)
    early_state = kernel(near_early, STATE, 16, 4 * QUERIES * PROMPT_TOKENS * HEAD_SIZE)(*early, prompt_cache)

    spread, early_state = lax.optimization_barrier((spread, early_state))
    shape = (nodes, 2 * spread.shape[1] + SPARE, HEAD_SIZE)
    picked = kernel(pick, [(shape, BF16)], 16, 1 << 22, (), [SMEM, SMEM, VMEM])(parents, leaf_scores, spread)[0]
    context = lax.all_to_all(picked, "branch", 0, 0, tiled=True)
    other_weight = tensor(output_weight, SWAP)

    late = run_project(1, x4, x3, x7, x6)
    depth = output_weight.shape[0]
    state = kernel(near_late, STATE + STATE, 20, 4 * QUERIES * (PROMPT_TOKENS + 2 * SEGMENT_TOKENS) * HEAD_SIZE)(
        prompt_cache, *early, *early_state, *late
    )

    halves = [((ROWS // 2, 3 * HEAD_SIZE), BF16)] * 2
    run_far = kernel(far, halves, 16, 4 * QUERIES * 2 * SEGMENT_TOKENS * HEAD_SIZE)
    depth = output_weight.shape[0]

    def run_output(first, count, a, b):
        return kernel(
            functools.partial(output, first, count // 2),
            [((BLOCK, count), BF16)] * 2,
            OUTPUT_MIB,
            8 * BLOCK * depth * count,
            [pltpu.VMEM((2 * depth, count), BF16), pltpu.SemaphoreType.DMA((4,))],
            [VMEM, VMEM, ANY, ANY],
        )(a, b, output_weight, other_weight)

    half = features // 2
    late_mine, late_other = run_far(late[0], context, *state[3:])
    late_came = tensor(late_other, SWAP)
    early_mine, early_other = run_far(early[0], context, *state[:3])
    early_came = tensor(early_other, SWAP)
    z1, z2 = [], []
    for i in range(2):
        y4, y3 = run_output(i * half, half, late_mine, late_came)
        z2.append(tensor(y4, BACK))
        z1.append(tensor(y3, BACK))
    y2, y0 = run_output(0, features, early_mine, early_came)
    y2 = kernel(join, [((BLOCK, features), BF16)], 8, 1 << 20)(y2, *z2)[0]
    z0 = tensor(y2, BACK)
    least, product = kernel(tree, [((2, 1), F32)] * 2, 8, 1 << 20, (), [SMEM, VMEM])(parents, context)
    z1 = [tensor(part, SWAP) for part in z1]
    own = kernel(join, [((BLOCK, features), F32)], 8, 1 << 20)(y0, *z1)[0]
    attn_output = (own + z0.astype(F32)).astype(BF16)
    return attn_output, least, product


def solution(mesh):
    placed = (
        P(("branch", "tensor"), None),
        P(),
        P(None, "tensor"),
        P("tensor", None),
        P(None, "tensor"),
        P(None, "branch", "tensor"),
        P(),
        P("branch"),
    )
    return jax.shard_map(
        per_device,
        mesh=mesh,
        in_specs=placed,
        out_specs=(P(("branch", "tensor"), None), P(None, "branch"), P(None, "branch")),
        check_vma=False,
    )
```
